32 devices in a mesh: blk: 16 (over z, x, core), own: 2 (over y).
Axes of the slice: x: 2, y: 2, z: 4, core: 2. Of those that a mesh axis runs over, the one named last changes fastest.
Arguments:
- embeddings: bfloat16 [4096, 768], P(('blk', 'own')), may hold values from -320 to 320
- centroids: bfloat16 [16384, 768], P('blk'), may hold values from -4 to 4
- log_weight: float32 [16384], P('blk'), may hold values from -0.5 to 1.6
Outputs:
- new_centroids: float32 [16384, 768], P(('blk', 'own'))
- counts: float32 [16384], P(('blk', 'own'))
- log_norm: float32 [4096], P(('blk', 'own'))
The draws below stay inside these ranges and needn't reach their ends.
All inputs are finite; a program needn't handle non-finite values.
Results may differ from the reference program's by a relative error of at most 0.0015.
Values may be sent and summed in bfloat16 or wider, within the bound.
A program may use at most 64 MiB of HBM per device.

```python
import math
import jax
import jax.numpy as jnp
from jax import lax

D = 768
K = 16384
ROWS = 4096


def centre_base(key):
    values = jax.random.normal(jax.random.fold_in(key, 101), (K, D), jnp.float32)
    return jnp.clip(values, -4.0, 4.0)


def weight_base(key):
    place = jnp.arange(K, dtype=jnp.float32) / K
    noise = jax.random.uniform(jax.random.fold_in(key, 303), (K,), jnp.float32, -0.5, 0.5)
    return jnp.log(1.0 + 2.0 * place) + noise


def draw_centroids(key, part):
    return centre_base(key).astype(jnp.bfloat16)


def draw_log_weight(key, part):
    return weight_base(key)


def draw_embeddings(key, part):
    values = jax.random.normal(jax.random.fold_in(key, 202), (ROWS, D), jnp.float32)
    values = jnp.clip(values, -5.0, 5.0)
    return values.astype(jnp.bfloat16)


def setup_inputs(seed: int = 0) -> dict:
    arg_keys = jax.random.split(jax.random.key(seed), 4)
    embeddings = draw_embeddings(jax.random.fold_in(arg_keys[3], 71), 0)
    centroids = draw_centroids(jax.random.fold_in(arg_keys[3], 71), 0)
    log_weight = draw_log_weight(jax.random.fold_in(arg_keys[3], 71), 0)
    return dict(embeddings=embeddings, centroids=centroids, log_weight=log_weight)


prior_mass = 1.0

def score_rows(row_block, centroids, half_sq, log_weight, scale_root):
    dots = jnp.dot(row_block, centroids.T, preferred_element_type=jnp.float32)
    return (dots - half_sq[None, :]) / scale_root + log_weight[None, :]

def reference(embeddings, centroids, log_weight):
    row_count = embeddings.shape[0]
    block_len = math.gcd(row_count, 1024)
    centre_vals = centroids.astype(jnp.float32)
    half_sq = 0.5 * lax.optimization_barrier(jnp.sum(centre_vals * centre_vals, axis=1))
    scale_root = math.sqrt(D)
    row_blocks = embeddings.reshape(row_count // block_len, block_len, D)

    def advance(running, row_block):
        weighted, counts = running
        logits = score_rows(row_block, centroids, half_sq, log_weight, scale_root)
        peak_val = lax.optimization_barrier(jnp.max(logits, axis=1))
        mass_sum = lax.optimization_barrier(jnp.sum(jnp.exp(logits - peak_val[:, None]), axis=1))
        log_total = peak_val + jnp.log(mass_sum)
        resp_vals = jnp.exp(logits - log_total[:, None])
        counts = counts + lax.optimization_barrier(jnp.sum(resp_vals, axis=0))
        weighted = weighted + jnp.dot(resp_vals.astype(jnp.bfloat16).T, row_block, preferred_element_type=jnp.float32)
        return ((weighted, counts), log_total)
    start_pair = (jnp.zeros((K, D), jnp.float32), jnp.zeros((K,), jnp.float32))
    (weighted, counts), log_total = lax.scan(advance, start_pair, row_blocks)
    updated = (weighted + prior_mass * centre_vals) / (counts[:, None] + prior_mass)
    return (updated, counts, log_total.reshape(row_count))
```

```python
import functools
import math

import jax
import jax.numpy as jnp
from jax import lax
from jax.experimental import pallas as pl
from jax.experimental.pallas import tpu as pltpu
from jax.sharding import PartitionSpec as P

prior_mass = 1.0
MESH = pl.DeviceIdType.MESH
PIECES = 4
LANES = 128


def merged(value, axis, join):
    pieces = jax.tree.map(lambda part: lax.all_gather(part, axis), value)
    head = jax.tree.map(lambda part: part[0], pieces)
    tail = jax.tree.map(lambda part: part[1:], pieces)
    running, _ = lax.scan(lambda running, share: (join(running, share), None), head, tail)
    return running


def score_rows(row_block, centroids, half_sq, log_weight, scale_root):
    dots = lax.dot_general(
        row_block, centroids, (((1,), (1,)), ((), ())), preferred_element_type=jnp.float32
    )
    return (dots - half_sq[None, :]) / scale_root + log_weight[None, :]


def local(embeddings, centroids, log_weight):
    row_count, feat_dim = embeddings.shape
    local_count = centroids.shape[0]
    centre_vals = centroids.astype(jnp.float32)
    half_sq = 0.5 * jnp.sum(centre_vals * centre_vals, axis=1)
    scale_root = math.sqrt(feat_dim)
    groups = lax.axis_size("blk")
    gathered_count = row_count * groups
    block_len = math.gcd(gathered_count, 1024)

    def block_terms(row_block, log_part):
        logits = score_rows(row_block, centroids, half_sq, log_weight, scale_root)
        resp_vals = jnp.exp(logits - log_part[:, None])
        contrib = lax.dot_general(
            resp_vals.astype(jnp.bfloat16),
            row_block,
            (((0,), (0,)), ((), ())),
            preferred_element_type=jnp.float32,
        )
        return (contrib, jnp.sum(resp_vals, axis=0))

    shard_rows = lax.all_gather(embeddings, "blk", axis=0, tiled=True)
    logits = score_rows(shard_rows, centroids, half_sq, log_weight, scale_root)
    peak_val = jnp.max(logits, axis=1)
    peak_part = peak_val
    mass_part = jnp.sum(jnp.exp(logits - peak_val[:, None]), axis=1)
    peak_val = peak_part
    mass_sum = mass_part

    def combine(first_pair, later_pair):
        joined = jnp.maximum(first_pair[0], later_pair[0])
        return (
            joined,
            first_pair[1] * jnp.exp(first_pair[0] - joined)
            + later_pair[1] * jnp.exp(later_pair[0] - joined),
        )

    peak_val, mass_sum = merged((peak_val, mass_sum), "blk", combine)
    log_total = peak_val + jnp.log(mass_sum)
    empty_sums = jnp.zeros((local_count, feat_dim), jnp.float32)
    empty_counts = jnp.zeros((local_count,), jnp.float32)

    def advance(running, inputs):
        contrib, count_part = block_terms(inputs[0], inputs[1])
        return ((running[0] + contrib, running[1] + count_part), None)

    row_blocks = shard_rows.reshape(gathered_count // block_len, block_len, feat_dim)
    log_blocks = log_total.reshape(gathered_count // block_len, block_len)
    (weighted, counts), unused = lax.scan(
        advance, (empty_sums, empty_counts), (row_blocks, log_blocks)
    )
    weighted, counts = (
        lax.psum_scatter(weighted, "own", scatter_dimension=0, tiled=True),
        lax.psum_scatter(counts, "own", scatter_dimension=0, tiled=True),
    )
    owned_count = local_count // lax.axis_size("own")
    own_index = lax.axis_index("own")
    own_centres = lax.dynamic_slice_in_dim(centre_vals, own_index * owned_count, owned_count, 0)
    updated = (weighted + prior_mass * own_centres) / (counts[:, None] + prior_mass)
    log_norm = lax.dynamic_slice_in_dim(log_total, lax.axis_index("blk") * row_count, row_count, 0)
    return (updated, counts, log_norm)


def row_to_column(row):
    eye = lax.broadcasted_iota(jnp.int32, (LANES, LANES), 0) == lax.broadcasted_iota(
        jnp.int32, (LANES, LANES), 1
    )
    return jnp.sum(jnp.where(eye, jnp.broadcast_to(row, (LANES, LANES)), 0.0), axis=1, keepdims=True)


def column_to_row(column):
    eye = lax.broadcasted_iota(jnp.int32, (LANES, LANES), 0) == lax.broadcasted_iota(
        jnp.int32, (LANES, LANES), 1
    )
    return jnp.sum(
        jnp.where(eye, jnp.broadcast_to(column, (LANES, LANES)), 0.0), axis=0, keepdims=True
    )


def join_logs(parts):
    top = functools.reduce(jnp.maximum, parts)
    return top + jnp.log2(sum(jnp.exp2(part - top) for part in parts))


def kernel(
    depth,
    x_ref,
    c_hbm,
    lw_ref,
    new_ref,
    counts_ref,
    log_ref,
    xall,
    cen,
    bias,
    expd,
    peaks,
    resp,
    total,
    mass,
    stat1,
    got1,
    stat2,
    got2,
    sem_in,
    send_z,
    recv_z,
    send_x,
    recv_x,
    send_y,
    recv_y,
    send_dx,
    recv_dx,
    send_dy,
    recv_dy,
    send_c,
    recv_c,
    send_s1,
    recv_s1,
    send_s2,
    recv_s2,
):
    blk, own = lax.axis_index("blk"), lax.axis_index("own")
    core = blk % 2
    px = (blk // 2) % 2
    qz = blk // 4
    local_count, feat = cen.shape
    per = x_ref.shape[0] // PIECES
    half = per // 2
    piece_rows = xall.shape[1]
    sub = piece_rows // depth
    tiles = sub // LANES
    log2e = math.log2(math.e)

    def device(q, p, o, c):
        return ((q * 2 + p) * 2 + c, o)

    def slot(q, p, o, c):
        return ((q * 2 + p) * 2 + o) * 2 + c

    def rows_of(j, q, p, o, c, start=0, count=None):
        first = pl.multiple_of(slot(q, p, o, c) * per + start, half)
        return xall.at[j, pl.ds(first, per if count is None else count), :]

    def zback(d):
        return (qz + depth - d) % depth

    x_dev = device(qz, 1 - px, own, core)
    y_dev = device(qz, px, 1 - own, core)
    c_dev = device(qz, px, own, 1 - core)
    z_devs = [None] + [device((qz + d) % depth, px, own, core) for d in range(1, depth)]
    plane = [None]
    for mask in range(1, 8):
        p = 1 - px if mask & 1 else px
        o = 1 - own if mask & 2 else own
        c = 1 - core if mask & 4 else core
        plane.append(device(qz, p, o, c))
    started = []

    def push(src, dst, send, recv, dev):
        copy = pltpu.make_async_remote_copy(
            src_ref=src, dst_ref=dst, send_sem=send, recv_sem=recv, device_id=dev, device_id_type=MESH
        )
        copy.start()
        started.append(copy)

    def arrive(dst, recv):
        pltpu.make_async_remote_copy(
            src_ref=dst, dst_ref=dst, send_sem=recv, recv_sem=recv, device_id=x_dev, device_id_type=MESH
        ).wait_recv()

    first_row = pl.multiple_of(own * local_count, local_count)
    cen_copy = pltpu.make_async_copy(c_hbm.at[pl.ds(first_row, local_count), :], cen, sem_in.at[0])
    cen_copy.start()
    own_copies = []
    for j in range(PIECES):
        copy = pltpu.make_async_copy(
            x_ref.at[pl.ds(j * per, per), :], rows_of(j, qz, px, own, core), sem_in.at[1 + j]
        )
        copy.start()
        own_copies.append(copy)

    barrier = pltpu.get_barrier_semaphore()
    partners = z_devs[1:] + plane[1:]
    for dev in partners:
        pl.semaphore_signal(barrier, inc=1, device_id=dev, device_id_type=MESH)
    pl.semaphore_wait(barrier, len(partners))

    def send_own(j):
        src = x_ref.at[pl.ds(j * per, per), :]
        dst = rows_of(j, qz, px, own, core)
        push(src, dst, send_x.at[j, 0], recv_x.at[j, 0], x_dev)
        push(src, dst, send_y.at[j, 0], recv_y.at[j, 0], y_dev)
        for d in range(1, depth):
            push(src, dst, send_z.at[j, d], recv_z.at[j, d], z_devs[d])
        push(src, dst, send_c.at[j, 0, 0], recv_c.at[j, 0, 0], c_dev)

    def on_z(j, d):
        block = rows_of(j, zback(d), px, own, core)
        arrive(block, recv_z.at[j, d])
        push(block, block, send_x.at[j, d], recv_x.at[j, d], x_dev)
        push(block, block, send_y.at[j, d], recv_y.at[j, d], y_dev)
        push(block, block, send_c.at[j, 0, d], recv_c.at[j, 0, d], c_dev)

    def on_xy(j, d):
        q = zback(d)
        block = rows_of(j, q, 1 - px, own, core)
        arrive(block, recv_x.at[j, d])
        part = rows_of(j, q, 1 - px, own, core, 0, half)
        push(part, part, send_dy.at[j, d], recv_dy.at[j, d], y_dev)
        push(block, block, send_c.at[j, 1, d], recv_c.at[j, 1, d], c_dev)
        block = rows_of(j, q, px, 1 - own, core)
        arrive(block, recv_y.at[j, d])
        part = rows_of(j, q, px, 1 - own, core, half, half)
        push(part, part, send_dx.at[j, d], recv_dx.at[j, d], x_dev)
        push(block, block, send_c.at[j, 2, d], recv_c.at[j, 2, d], c_dev)

    def on_diag(j, d):
        q = zback(d)
        arrive(rows_of(j, q, 1 - px, 1 - own, core, 0, half), recv_dy.at[j, d])
        arrive(rows_of(j, q, 1 - px, 1 - own, core, half, half), recv_dx.at[j, d])
        block = rows_of(j, q, 1 - px, 1 - own, core)
        push(block, block, send_c.at[j, 3, d], recv_c.at[j, 3, d], c_dev)

    def on_core(j):
        own_copies[j].wait()
        for d in range(depth):
            q = zback(d)
            for kind, (p, o) in enumerate(
                ((px, own), (1 - px, own), (px, 1 - own), (1 - px, 1 - own))
            ):
                arrive(rows_of(j, q, p, o, 1 - core), recv_c.at[j, kind, d])

    def arrivals(j):
        groups = []
        for t in range(depth):
            def group(t=t):
                if t == 0 and j + 1 < PIECES:
                    send_own(j + 1)
                if t == 0 and depth > 1:
                    on_z(j, 1)
                if t + 2 < depth:
                    on_z(j, t + 2)
                on_xy(j, t)
                if t >= 1:
                    on_diag(j, t - 1)
                if t == depth - 1:
                    on_diag(j, t)
                    on_core(j)
            groups.append(group)
        return groups

    def first_pass(j, t):
        rows = xall[j, pl.ds(t * sub, sub), :]
        dots = lax.dot_general(
            cen[...], rows, (((1,), (1,)), ((), ())), preferred_element_type=jnp.float32
        )
        logits = dots * (log2e / math.sqrt(feat)) + bias[...]
        peak = jnp.max(logits, axis=0, keepdims=True)
        vals = jnp.exp2(logits - peak)
        expd[j, t] = vals
        peaks[j, t] = peak
        logs = peak + jnp.log2(jnp.sum(vals, axis=0, keepdims=True))
        for i in range(tiles):
            stat1[j, pl.ds(t * tiles + i, 1), :] = logs[:, i * LANES : (i + 1) * LANES]

    def stats_send(j):
        for mask in range(1, 8):
            push(
                stat1.at[j], got1.at[j, mask], send_s1.at[j, mask], recv_s1.at[j, mask], plane[mask]
            )

    def stats_mid(j):
        for mask in range(1, 8):
            arrive(got1.at[j, mask], recv_s1.at[j, mask])
        stat2[j] = join_logs([stat1[j]] + [got1[j, mask] for mask in range(1, 8)])
        for d in range(1, depth):
            push(stat2.at[j], got2.at[j, d], send_s2.at[j, d], recv_s2.at[j, d], z_devs[d])

    def stats_end(j):
        for d in range(1, depth):
            arrive(got2.at[j, d], recv_s2.at[j, d])
        log_ref[j] = join_logs([stat2[j]] + [got2[j, d] for d in range(1, depth)])

    def second_pass(j, part, parts):
        width = depth // parts
        for t in range(part * width, (part + 1) * width):
            norm = jnp.concatenate(
                [log_ref[j, pl.ds(t * tiles + i, 1), :] for i in range(tiles)], axis=1
            )
            vals = expd[j, t] * jnp.exp2(peaks[j, t] - norm)
            mass[...] += sum(vals[:, i * LANES : (i + 1) * LANES] for i in range(tiles))
            k = t - part * width
            resp[:, k * sub : (k + 1) * sub] = vals.astype(jnp.bfloat16)
        span = width * sub
        total[...] += jnp.dot(
            resp[:, :span],
            xall[j, pl.ds(part * span, span), :],
            preferred_element_type=jnp.float32,
        )

    send_own(0)
    cen_copy.wait()
    total[...] = jnp.zeros_like(total)
    mass[...] = jnp.zeros_like(mass)
    for i in range(local_count // LANES):
        span = pl.ds(i * LANES, LANES)
        vals = cen[span, :].astype(jnp.float32)
        half_sq = 0.5 * jnp.sum(vals * vals, axis=1, keepdims=True)
        weight = row_to_column(lw_ref[pl.ds(own * (local_count // LANES) + i, 1), :])
        column = (weight - half_sq / math.sqrt(feat)) * log2e
        bias[span, :] = jnp.broadcast_to(column, (LANES, sub))
    for group in arrivals(0):
        group()
    for j in range(PIECES):
        groups = arrivals(j + 1) if j + 1 < PIECES else []
        for t in range(depth):
            if groups:
                groups[t]()
            first_pass(j, t)
            if j >= 1 and t == depth // 2 - 1:
                stats_mid(j - 1)
            if j >= 1 and t == depth - 1:
                stats_end(j - 1)
            if j >= 2 and t % 2 == 0:
                second_pass(j - 2, t // 2, depth // 2)
        stats_send(j)
    last = PIECES - 1
    second_pass(last - 1, 0, 2)
    stats_mid(last)
    second_pass(last - 1, 1, 2)
    stats_end(last)
    second_pass(last, 0, 2)
    second_pass(last, 1, 2)
    for i in range(local_count // LANES):
        span = pl.ds(i * LANES, LANES)
        counts = jnp.sum(mass[span, :], axis=1, keepdims=True)
        counts_ref[pl.ds(i, 1), :] = column_to_row(counts)
        new_ref[span, :] = (total[span, :] + prior_mass * cen[span, :].astype(jnp.float32)) / (
            counts + prior_mass
        )
    for copy in started:
        copy.wait_send()


def fused(blk_size, own_size, embeddings, centroids, log_weight):
    row_count, feat = embeddings.shape
    local_count = centroids.shape[0] // own_size
    depth = blk_size // 4
    piece_rows = row_count * blk_size * own_size // PIECES
    vmem = PIECES * piece_rows * (feat * 2 + local_count * 4)
    fits = (
        own_size == 2
        and blk_size % 16 == 0
        and row_count % (32 * PIECES) == 0
        and local_count % LANES == 0
        and centroids.shape[0] % LANES == 0
        and vmem < 40 * 2**20
    )
    if not fits:
        return local(embeddings, centroids, log_weight)
    sub = piece_rows // depth
    tile = (PIECES, piece_rows // LANES, LANES)
    dma = pltpu.SemaphoreType.DMA
    vm = pl.BlockSpec(memory_space=pltpu.VMEM)
    updated, counts, logs = pl.pallas_call(
        functools.partial(kernel, depth),
        out_shape=(
            jax.ShapeDtypeStruct((local_count, feat), jnp.float32),
            jax.ShapeDtypeStruct((local_count // LANES, LANES), jnp.float32),
            jax.ShapeDtypeStruct(tile, jnp.float32),
        ),
        in_specs=[vm, pl.BlockSpec(memory_space=pl.ANY), vm],
        out_specs=(vm, vm, vm),
        scratch_shapes=[
            pltpu.VMEM((PIECES, piece_rows, feat), jnp.bfloat16),
            pltpu.VMEM((local_count, feat), jnp.bfloat16),
            pltpu.VMEM((local_count, sub), jnp.float32),
            pltpu.VMEM((PIECES, depth, local_count, sub), jnp.float32),
            pltpu.VMEM((PIECES, depth, 1, sub), jnp.float32),
            pltpu.VMEM((local_count, piece_rows // 2), jnp.bfloat16),
            pltpu.VMEM((local_count, feat), jnp.float32),
            pltpu.VMEM((local_count, LANES), jnp.float32),
            pltpu.VMEM(tile, jnp.float32),
            pltpu.VMEM((PIECES, 8) + tile[1:], jnp.float32),
            pltpu.VMEM(tile, jnp.float32),
            pltpu.VMEM((PIECES, depth) + tile[1:], jnp.float32),
            dma((1 + PIECES,)),
        ]
        + [dma((PIECES, depth))] * 10
        + [dma((PIECES, 4, depth))] * 2
        + [dma((PIECES, 8))] * 2
        + [dma((PIECES, depth))] * 2,
        compiler_params=pltpu.CompilerParams(
            collective_id=0, has_side_effects=True, vmem_limit_bytes=56 * 2**20
        ),
    )(embeddings, centroids, log_weight.reshape(-1, LANES))
    place = lax.axis_index("blk")
    spot = ((place // 2) * own_size + lax.axis_index("own")) * 2 + place % 2
    mine = lax.dynamic_slice_in_dim(
        logs.reshape(PIECES, blk_size * own_size, row_count // PIECES), spot, 1, 1
    )
    return (updated, counts.reshape(-1), mine.reshape(-1) * math.log(2.0))


def solution(mesh):
    placed = (P(("blk", "own"), None), P("blk", None), P("blk"))
    return jax.shard_map(
        functools.partial(fused, mesh.shape["blk"], mesh.shape["own"]),
        mesh=mesh,
        in_specs=placed,
        out_specs=(P(("blk", "own"), None), P(("blk", "own")), P(("blk", "own"))),
        check_vma=False,
    )
```

```python
import functools
import math

import jax
import jax.numpy as jnp
from jax import lax
from jax.experimental import pallas as pl
from jax.experimental.pallas import tpu as pltpu
from jax.sharding import PartitionSpec as P

prior_mass = 1.0
MESH = pl.DeviceIdType.MESH
PIECES = 4
AHEAD = 2
LANES = 128


def merged(value, axis, join):
    pieces = jax.tree.map(lambda part: lax.all_gather(part, axis), value)
    head = jax.tree.map(lambda part: part[0], pieces)
    tail = jax.tree.map(lambda part: part[1:], pieces)
    running, _ = lax.scan(lambda running, share: (join(running, share), None), head, tail)
    return running


def score_rows(row_block, centroids, half_sq, log_weight, scale_root):
    dots = lax.dot_general(
        row_block, centroids, (((1,), (1,)), ((), ())), preferred_element_type=jnp.float32
    )
    return (dots - half_sq[None, :]) / scale_root + log_weight[None, :]


def local(embeddings, centroids, log_weight):
    row_count, feat_dim = embeddings.shape
    local_count = centroids.shape[0]
    centre_vals = centroids.astype(jnp.float32)
    half_sq = 0.5 * jnp.sum(centre_vals * centre_vals, axis=1)
    scale_root = math.sqrt(feat_dim)
    groups = lax.axis_size("blk")
    gathered_count = row_count * groups
    block_len = math.gcd(gathered_count, 1024)

    def block_terms(row_block, log_part):
        logits = score_rows(row_block, centroids, half_sq, log_weight, scale_root)
        resp_vals = jnp.exp(logits - log_part[:, None])
        contrib = lax.dot_general(
            resp_vals.astype(jnp.bfloat16),
            row_block,
            (((0,), (0,)), ((), ())),
            preferred_element_type=jnp.float32,
        )
        return (contrib, jnp.sum(resp_vals, axis=0))

    shard_rows = lax.all_gather(embeddings, "blk", axis=0, tiled=True)
    logits = score_rows(shard_rows, centroids, half_sq, log_weight, scale_root)
    peak_val = jnp.max(logits, axis=1)
    peak_part = peak_val
    mass_part = jnp.sum(jnp.exp(logits - peak_val[:, None]), axis=1)
    peak_val = peak_part
    mass_sum = mass_part

    def combine(first_pair, later_pair):
        joined = jnp.maximum(first_pair[0], later_pair[0])
        return (
            joined,
            first_pair[1] * jnp.exp(first_pair[0] - joined)
            + later_pair[1] * jnp.exp(later_pair[0] - joined),
        )

    peak_val, mass_sum = merged((peak_val, mass_sum), "blk", combine)
    log_total = peak_val + jnp.log(mass_sum)
    empty_sums = jnp.zeros((local_count, feat_dim), jnp.float32)
    empty_counts = jnp.zeros((local_count,), jnp.float32)

    def advance(running, inputs):
        contrib, count_part = block_terms(inputs[0], inputs[1])
        return ((running[0] + contrib, running[1] + count_part), None)

    row_blocks = shard_rows.reshape(gathered_count // block_len, block_len, feat_dim)
    log_blocks = log_total.reshape(gathered_count // block_len, block_len)
    (weighted, counts), unused = lax.scan(
        advance, (empty_sums, empty_counts), (row_blocks, log_blocks)
    )
    weighted, counts = (
        lax.psum_scatter(weighted, "own", scatter_dimension=0, tiled=True),
        lax.psum_scatter(counts, "own", scatter_dimension=0, tiled=True),
    )
    owned_count = local_count // lax.axis_size("own")
    own_index = lax.axis_index("own")
    own_centres = lax.dynamic_slice_in_dim(centre_vals, own_index * owned_count, owned_count, 0)
    updated = (weighted + prior_mass * own_centres) / (counts[:, None] + prior_mass)
    log_norm = lax.dynamic_slice_in_dim(log_total, lax.axis_index("blk") * row_count, row_count, 0)
    return (updated, counts, log_norm)


def row_to_column(row):
    eye = lax.broadcasted_iota(jnp.int32, (LANES, LANES), 0) == lax.broadcasted_iota(
        jnp.int32, (LANES, LANES), 1
    )
    return jnp.sum(jnp.where(eye, jnp.broadcast_to(row, (LANES, LANES)), 0.0), axis=1, keepdims=True)


def column_to_row(column):
    eye = lax.broadcasted_iota(jnp.int32, (LANES, LANES), 0) == lax.broadcasted_iota(
        jnp.int32, (LANES, LANES), 1
    )
    return jnp.sum(
        jnp.where(eye, jnp.broadcast_to(column, (LANES, LANES)), 0.0), axis=0, keepdims=True
    )


def join_logs(parts):
    top = functools.reduce(jnp.maximum, parts)
    return top + jnp.log2(sum(jnp.exp2(part - top) for part in parts))


def kernel(
    depth,
    x_ref,
    c_hbm,
    lw_ref,
    new_ref,
    counts_ref,
    log_ref,
    xall,
    cen,
    bias,
    expd,
    peaks,
    resp,
    total,
    mass,
    stat1,
    got1,
    stat2,
    got2,
    sem_in,
    send_z,
    recv_z,
    send_x,
    recv_x,
    send_y,
    recv_y,
    send_dx,
    recv_dx,
    send_dy,
    recv_dy,
    send_c,
    recv_c,
    send_s1,
    recv_s1,
    send_s2,
    recv_s2,
):
    blk, own = lax.axis_index("blk"), lax.axis_index("own")
    core = blk % 2
    px = (blk // 2) % 2
    qz = blk // 4
    local_count, feat = cen.shape
    per = x_ref.shape[0] // PIECES
    half = per // 2
    piece_rows = xall.shape[1]
    sub = piece_rows // depth
    tiles = sub // LANES
    log2e = math.log2(math.e)

    def device(q, p, o, c):
        return ((q * 2 + p) * 2 + c, o)

    def slot(q, p, o, c):
        return ((q * 2 + p) * 2 + o) * 2 + c

    def rows_of(j, q, p, o, c, start=0, count=None):
        first = pl.multiple_of(slot(q, p, o, c) * per + start, half)
        return xall.at[j, pl.ds(first, per if count is None else count), :]

    def zback(d):
        return (qz + depth - d) % depth

    x_dev = device(qz, 1 - px, own, core)
    y_dev = device(qz, px, 1 - own, core)
    c_dev = device(qz, px, own, 1 - core)
    z_devs = [None] + [device((qz + d) % depth, px, own, core) for d in range(1, depth)]
    plane = [None]
    for mask in range(1, 8):
        p = 1 - px if mask & 1 else px
        o = 1 - own if mask & 2 else own
        c = 1 - core if mask & 4 else core
        plane.append(device(qz, p, o, c))
    started = []

    def push(src, dst, send, recv, dev):
        copy = pltpu.make_async_remote_copy(
            src_ref=src, dst_ref=dst, send_sem=send, recv_sem=recv, device_id=dev, device_id_type=MESH
        )
        copy.start()
        started.append(copy)

    def arrive(dst, recv):
        pltpu.make_async_remote_copy(
            src_ref=dst, dst_ref=dst, send_sem=recv, recv_sem=recv, device_id=x_dev, device_id_type=MESH
        ).wait_recv()

    first_row = pl.multiple_of(own * local_count, local_count)
    cen_copy = pltpu.make_async_copy(c_hbm.at[pl.ds(first_row, local_count), :], cen, sem_in.at[0])
    cen_copy.start()
    own_copies = []
    for j in range(PIECES):
        copy = pltpu.make_async_copy(
            x_ref.at[pl.ds(j * per, per), :], rows_of(j, qz, px, own, core), sem_in.at[1 + j]
        )
        copy.start()
        own_copies.append(copy)

    barrier = pltpu.get_barrier_semaphore()
    partners = z_devs[1:] + plane[1:]
    for dev in partners:
        pl.semaphore_signal(barrier, inc=1, device_id=dev, device_id_type=MESH)
    pl.semaphore_wait(barrier, len(partners))

    def send_own(j):
        src = x_ref.at[pl.ds(j * per, per), :]
        dst = rows_of(j, qz, px, own, core)
        push(src, dst, send_x.at[j, 0], recv_x.at[j, 0], x_dev)
        push(src, dst, send_y.at[j, 0], recv_y.at[j, 0], y_dev)
        for d in range(1, depth):
            push(src, dst, send_z.at[j, d], recv_z.at[j, d], z_devs[d])
        push(src, dst, send_c.at[j, 0, 0], recv_c.at[j, 0, 0], c_dev)

    def on_z(j, d):
        block = rows_of(j, zback(d), px, own, core)
        arrive(block, recv_z.at[j, d])
        push(block, block, send_x.at[j, d], recv_x.at[j, d], x_dev)
        push(block, block, send_y.at[j, d], recv_y.at[j, d], y_dev)
        push(block, block, send_c.at[j, 0, d], recv_c.at[j, 0, d], c_dev)

    def on_xy(j, d):
        q = zback(d)
        block = rows_of(j, q, 1 - px, own, core)
        arrive(block, recv_x.at[j, d])
        part = rows_of(j, q, 1 - px, own, core, 0, half)
        push(part, part, send_dy.at[j, d], recv_dy.at[j, d], y_dev)
        push(block, block, send_c.at[j, 1, d], recv_c.at[j, 1, d], c_dev)
        block = rows_of(j, q, px, 1 - own, core)
        arrive(block, recv_y.at[j, d])
        part = rows_of(j, q, px, 1 - own, core, half, half)
        push(part, part, send_dx.at[j, d], recv_dx.at[j, d], x_dev)
        push(block, block, send_c.at[j, 2, d], recv_c.at[j, 2, d], c_dev)

    def on_diag(j, d):
        q = zback(d)
        arrive(rows_of(j, q, 1 - px, 1 - own, core, 0, half), recv_dy.at[j, d])
        arrive(rows_of(j, q, 1 - px, 1 - own, core, half, half), recv_dx.at[j, d])
        block = rows_of(j, q, 1 - px, 1 - own, core)
        push(block, block, send_c.at[j, 3, d], recv_c.at[j, 3, d], c_dev)

    def on_core(j):
        own_copies[j].wait()
        for d in range(depth):
            q = zback(d)
            for kind, (p, o) in enumerate(
                ((px, own), (1 - px, own), (px, 1 - own), (1 - px, 1 - own))
            ):
                arrive(rows_of(j, q, p, o, 1 - core), recv_c.at[j, kind, d])

    def stage(k):
        steps = []
        if k < PIECES:
            steps += [lambda: on_xy(k, 0)]
            steps += [functools.partial(on_z, k, d) for d in range(1, depth)]
        if 0 <= k - 2 < PIECES:
            steps += [functools.partial(on_diag, k - 2, d) for d in range(depth)]
        if 0 <= k - 1 < PIECES:
            steps += [functools.partial(on_xy, k - 1, d) for d in range(1, depth)]
        if 0 <= k - 2 < PIECES:
            steps += [lambda: on_core(k - 2)]
        size = -(-len(steps) // depth)
        return [steps[t * size : (t + 1) * size] for t in range(depth)]

    def first_pass(j, t):
        rows = xall[j, pl.ds(t * sub, sub), :]
        dots = lax.dot_general(
            cen[...], rows, (((1,), (1,)), ((), ())), preferred_element_type=jnp.float32
        )
        logits = dots * (log2e / math.sqrt(feat)) + bias[...]
        peak = jnp.max(logits, axis=0, keepdims=True)
        vals = jnp.exp2(logits - peak)
        expd[j, t] = vals
        peaks[j, t] = peak
        logs = peak + jnp.log2(jnp.sum(vals, axis=0, keepdims=True))
        for i in range(tiles):
            stat1[j, pl.ds(t * tiles + i, 1), :] = logs[:, i * LANES : (i + 1) * LANES]

    def stats_send(j):
        for mask in range(1, 8):
            push(
                stat1.at[j], got1.at[j, mask], send_s1.at[j, mask], recv_s1.at[j, mask], plane[mask]
            )

    def stats_mid(j):
        for mask in range(1, 8):
            arrive(got1.at[j, mask], recv_s1.at[j, mask])
        stat2[j] = join_logs([stat1[j]] + [got1[j, mask] for mask in range(1, 8)])
        for d in range(1, depth):
            push(stat2.at[j], got2.at[j, d], send_s2.at[j, d], recv_s2.at[j, d], z_devs[d])

    def stats_end(j):
        for d in range(1, depth):
            arrive(got2.at[j, d], recv_s2.at[j, d])
        log_ref[j] = join_logs([stat2[j]] + [got2[j, d] for d in range(1, depth)])

    def second_pass(j, part, parts):
        width = depth // parts
        for t in range(part * width, (part + 1) * width):
            norm = jnp.concatenate(
                [log_ref[j, pl.ds(t * tiles + i, 1), :] for i in range(tiles)], axis=1
            )
            vals = expd[j, t] * jnp.exp2(peaks[j, t] - norm)
            mass[...] += sum(vals[:, i * LANES : (i + 1) * LANES] for i in range(tiles))
            k = t - part * width
            resp[:, k * sub : (k + 1) * sub] = vals.astype(jnp.bfloat16)
        span = width * sub
        total[...] += jnp.dot(
            resp[:, :span],
            xall[j, pl.ds(part * span, span), :],
            preferred_element_type=jnp.float32,
        )

    for j in range(min(AHEAD, PIECES)):
        send_own(j)
    cen_copy.wait()
    total[...] = jnp.zeros_like(total)
    mass[...] = jnp.zeros_like(mass)
    for i in range(local_count // LANES):
        span = pl.ds(i * LANES, LANES)
        vals = cen[span, :].astype(jnp.float32)
        half_sq = 0.5 * jnp.sum(vals * vals, axis=1, keepdims=True)
        weight = row_to_column(lw_ref[pl.ds(own * (local_count // LANES) + i, 1), :])
        column = (weight - half_sq / math.sqrt(feat)) * log2e
        bias[span, :] = jnp.broadcast_to(column, (LANES, sub))
    lag = 3
    for k in range(PIECES + lag):
        if AHEAD <= k + AHEAD < PIECES:
            send_own(k + AHEAD)
        groups = stage(k)
        j = k - lag
        for t in range(depth):
            for step in groups[t]:
                step()
            if 0 <= j:
                first_pass(j, t)
            if j >= 1 and t == depth - 1:
                stats_mid(j - 1)
            if j >= 2 and t == 0:
                stats_end(j - 2)
            if j >= 2 and t % 2 == 0:
                second_pass(j - 2, t // 2, depth // 2)
        if 0 <= j:
            stats_send(j)
    last = PIECES - 1
    stats_end(last - 1)
    second_pass(last - 1, 0, 2)
    stats_mid(last)
    second_pass(last - 1, 1, 2)
    stats_end(last)
    second_pass(last, 0, 2)
    second_pass(last, 1, 2)
    for i in range(local_count // LANES):
        span = pl.ds(i * LANES, LANES)
        counts = jnp.sum(mass[span, :], axis=1, keepdims=True)
        counts_ref[pl.ds(i, 1), :] = column_to_row(counts)
        new_ref[span, :] = (total[span, :] + prior_mass * cen[span, :].astype(jnp.float32)) / (
            counts + prior_mass
        )
    for copy in started:
        copy.wait_send()


def fused(blk_size, own_size, embeddings, centroids, log_weight):
    row_count, feat = embeddings.shape
    local_count = centroids.shape[0] // own_size
    depth = blk_size // 4
    piece_rows = row_count * blk_size * own_size // PIECES
    vmem = PIECES * piece_rows * (feat * 2 + local_count * 4)
    fits = (
        own_size == 2
        and blk_size % 16 == 0
        and row_count % (32 * PIECES) == 0
        and local_count % LANES == 0
        and centroids.shape[0] % LANES == 0
        and vmem < 40 * 2**20
    )
    if not fits:
        return local(embeddings, centroids, log_weight)
    sub = piece_rows // depth
    tile = (PIECES, piece_rows // LANES, LANES)
    dma = pltpu.SemaphoreType.DMA
    vm = pl.BlockSpec(memory_space=pltpu.VMEM)
    updated, counts, logs = pl.pallas_call(
        functools.partial(kernel, depth),
        out_shape=(
            jax.ShapeDtypeStruct((local_count, feat), jnp.float32),
            jax.ShapeDtypeStruct((local_count // LANES, LANES), jnp.float32),
            jax.ShapeDtypeStruct(tile, jnp.float32),
        ),
        in_specs=[vm, pl.BlockSpec(memory_space=pl.ANY), vm],
        out_specs=(vm, vm, vm),
        scratch_shapes=[
            pltpu.VMEM((PIECES, piece_rows, feat), jnp.bfloat16),
            pltpu.VMEM((local_count, feat), jnp.bfloat16),
            pltpu.VMEM((local_count, sub), jnp.float32),
            pltpu.VMEM((PIECES, depth, local_count, sub), jnp.float32),
            pltpu.VMEM((PIECES, depth, 1, sub), jnp.float32),
            pltpu.VMEM((local_count, piece_rows // 2), jnp.bfloat16),
            pltpu.VMEM((local_count, feat), jnp.float32),
            pltpu.VMEM((local_count, LANES), jnp.float32),
            pltpu.VMEM(tile, jnp.float32),
            pltpu.VMEM((PIECES, 8) + tile[1:], jnp.float32),
            pltpu.VMEM(tile, jnp.float32),
            pltpu.VMEM((PIECES, depth) + tile[1:], jnp.float32),
            dma((1 + PIECES,)),
        ]
        + [dma((PIECES, depth))] * 10
        + [dma((PIECES, 4, depth))] * 2
        + [dma((PIECES, 8))] * 2
        + [dma((PIECES, depth))] * 2,
        compiler_params=pltpu.CompilerParams(
            collective_id=0, has_side_effects=True, vmem_limit_bytes=56 * 2**20
        ),
    )(embeddings, centroids, log_weight.reshape(-1, LANES))
    place = lax.axis_index("blk")
    spot = ((place // 2) * own_size + lax.axis_index("own")) * 2 + place % 2
    mine = lax.dynamic_slice_in_dim(
        logs.reshape(PIECES, blk_size * own_size, row_count // PIECES), spot, 1, 1
    )
    return (updated, counts.reshape(-1), mine.reshape(-1) * math.log(2.0))


def solution(mesh):
    placed = (P(("blk", "own"), None), P("blk", None), P("blk"))
    return jax.shard_map(
        functools.partial(fused, mesh.shape["blk"], mesh.shape["own"]),
        mesh=mesh,
        in_specs=placed,
        out_specs=(P(("blk", "own"), None), P(("blk", "own")), P(("blk", "own"))),
        check_vma=False,
    )
```
